32 devices in a mesh: dp: 8 (over z, x), mp: 4 (over y, core).
Axes of the slice: x: 2, y: 2, z: 4, core: 2. Of those that a mesh axis runs over, the one named last changes fastest.
Arguments:
- gating_logits: bfloat16 [8, 3, 64, 7168], P('dp', None, None, 'mp'), may hold values from -6 to 6
- lifted_hidden_values: bfloat16 [8, 3, 64, 7168], P('dp', None, None, 'mp'), may hold values from -6 to 6
- loss_output_grad: bfloat16 [8, 3, 64, 2048], P('dp', None, None, 'mp'), may hold values from -160 to 160
- arrival_flags: int32 [8], P('dp'), may hold values from 0 to 1, as said below
- block_owner_map: int32 [8, 3], P('dp'), may hold values from 0 to 7, as said below
- decoder_multipliers: int32 [8, 3], P('dp'), may hold values from 1 to 4
- block_piece_number: int32 [8], replicated, may hold values from 1 to 2, as said below
Outputs:
- down_grad: float32 [2048, 7168], P('dp', 'mp')
The draws below stay inside these ranges and needn't reach their ends.
Inputs may be any that keep to these rules, and one draw needn't show every extreme that they name: `arrival_flags`: at least one replica survives. `block_owner_map`: row i lists the partitions (i + r + k) mod 8 for k < 3, with one r for all rows. `block_piece_number`: some partition has exactly 2 live tiles.
All inputs are finite; a program needn't handle non-finite values.
Results may differ from the reference program's by a relative error of at most 0.0042.
Values may be sent and summed in bfloat16 or wider, within the bound.
No kernel may reach another device: no remote copies, remote signals or barrier semaphores. Data moves between devices by JAX's collectives and lax.ppermute only.
A program may use at most 128 MiB of HBM per device.

```python
import jax
import jax.numpy as jnp
from jax import lax

D = 2048
SLOTS = 3
TILE = 32
TILES = 2
TOK = 64
FF = 7168
N_DP = 8


def draw_arrival_flags(key, part):
    coin_flips = jax.random.randint(jax.random.fold_in(key, 11), (N_DP,), 0, 4)
    forced = jax.random.randint(jax.random.fold_in(key, 12), (), 0, N_DP)
    alive = jnp.where(coin_flips > 0, 1, 0)
    return jnp.where(jnp.arange(N_DP) == forced, 1, alive).astype(jnp.int32)


def draw_block_owner_map(key, part):
    rotation = jax.random.randint(jax.random.fold_in(key, 21), (), 0, N_DP)
    rows_idx = jnp.arange(N_DP, dtype=jnp.int32)[:, None]
    slot_idx = jnp.arange(SLOTS, dtype=jnp.int32)[None, :]
    return ((rows_idx + rotation + slot_idx) % N_DP).astype(jnp.int32)


def draw_block_piece_number(key, part):
    part_ids = jnp.arange(N_DP, dtype=jnp.int32)
    baseline = 1 + part_ids * (TILES - 1) // max(N_DP - 1, 1)
    jitter = jax.random.randint(jax.random.fold_in(key, 31), (N_DP,), 0, 2)
    return jnp.minimum(baseline + jitter, TILES).astype(jnp.int32)


def plant(array, own_key, low, high):
    shape = array.shape
    spot = [jax.random.randint(jax.random.fold_in(own_key, axis), (), 0, shape[axis]) for axis in range(len(shape))]
    array = array.at[tuple(spot)].set(low)
    longest = shape.index(max(shape))
    spot[longest] = (spot[longest] + 1) % shape[longest]
    return array.at[tuple(spot)].set(high)


def strengthened(entries, key, source, target, blocks, factor):
    owner, partner = [(jnp.arange(entries.shape[dim]) // (entries.shape[dim] // blocks)).reshape([-1 if axis == dim else 1 for axis in range(entries.ndim)]) for dim in (source, target)]
    chosen = jax.random.permutation(key, blocks)[partner]
    strong = (owner == chosen) | (owner == (partner + blocks // 2) % blocks)
    return jnp.where(strong, factor * entries, entries)


def shard_levels(own_key, extent, cuts, smallest, top_value):
    gain, own = 1.0, jax.random.fold_in(own_key, 6)
    for axis_at, blocks in cuts:
        steps = jnp.exp(jax.random.uniform(jax.random.fold_in(own, axis_at), (blocks,), jnp.float32, smallest / len(cuts), top_value / len(cuts)))
        gain = gain * jnp.repeat(steps, extent[axis_at] // blocks).reshape([-1 if axis == axis_at else 1 for axis in range(len(extent))])
    return gain


def normal_values(rng, dims, deviation, reach, cuts=(), held_as=jnp.bfloat16):
    result = deviation * jax.random.normal(rng, dims, jnp.float32)
    if cuts:
        result = result * shard_levels(rng, dims, cuts, -0.22, 0.18)
    return jnp.clip(result, -reach, reach).astype(held_as)


def noise_with(own_key, shape, scale, limit, cuts, heavy, held_as=jnp.bfloat16):
    result = scale * jax.random.normal(own_key, shape, jnp.float32)
    if cuts:
        result = result * shard_levels(own_key, shape, cuts, -0.22, 0.18)
    return jnp.clip(strengthened(result, jax.random.fold_in(own_key, 3), *heavy), -limit, limit).astype(held_as)


def setup_inputs(seed: int = 0) -> dict:
    key_of = jax.random.split(jax.random.key(seed), 8)
    return {
        "gating_logits": normal_values(key_of[0], (N_DP, SLOTS, TOK, FF), 1.0, 6.0, ((0, 8), (3, 4))),
        "lifted_hidden_values": normal_values(key_of[1], (N_DP, SLOTS, TOK, FF), 1.0, 6.0, ((0, 8), (3, 4))),
        "loss_output_grad": noise_with(key_of[2], (N_DP, SLOTS, TOK, D), ((N_DP * SLOTS * TOK) ** 0.5 / 2), 160.0, ((0, 8), (3, 4)), (0, 3, 8, 2.0)),
        "arrival_flags": draw_arrival_flags(jax.random.fold_in(key_of[7], 71), 0),
        "block_owner_map": draw_block_owner_map(jax.random.fold_in(key_of[7], 71), 0),
        "decoder_multipliers": plant(jax.random.randint(key_of[5], (N_DP, SLOTS), 1, 5), jax.random.fold_in(key_of[5], 1), 1, 4).astype(jnp.int32),
        "block_piece_number": draw_block_piece_number(jax.random.fold_in(key_of[7], 71), 0),
    }


def reference(gating_logits, lifted_hidden_values, loss_output_grad, arrival_flags, block_owner_map, decoder_multipliers, block_piece_number):
    part_ids = jnp.arange(N_DP, dtype=jnp.int32)
    slot_tiles = jnp.sum(jnp.where(block_owner_map[:, :, None] == part_ids[None, None, :], block_piece_number[None, None, :], 0), axis=2)
    live_rows = slot_tiles * TILE
    live_mask = jnp.arange(TOK, dtype=jnp.int32)[None, None, :] < live_rows[:, :, None]
    down_kernel_array = arrival_flags[:, None].astype(jnp.float32) * decoder_multipliers.astype(jnp.float32)
    total_tokens = jnp.sum(down_kernel_array * live_rows.astype(jnp.float32))

    def accumulate(running_total, current_inputs):
        gate_now, current_up_projection, cot_now, weight_now, live_now = current_inputs
        hidden = (jax.nn.silu(gate_now.astype(jnp.float32)) * current_up_projection.astype(jnp.float32) * live_now[:, :, None].astype(jnp.float32)).astype(jnp.bfloat16)
        scaled = hidden.astype(jnp.float32) * weight_now[:, None, None]
        contrib = jnp.einsum("ktd,ktf->df", cot_now.astype(jnp.float32), scaled, precision=lax.Precision.HIGHEST)
        return running_total + contrib, None

    start_sum = jnp.zeros((D, FF), jnp.float32)
    coded, _ = lax.scan(accumulate, start_sum, (gating_logits, lifted_hidden_values, loss_output_grad, down_kernel_array, live_mask))
    return coded / total_tokens
```

```python
import jax
import jax.numpy as jnp
from jax import lax
from jax.sharding import PartitionSpec as P

TILE = 32
CHUNKS = 2


def project(cots, hs):
    return lax.dot_general(cots, hs, (((0,), (0,)), ((), ())), preferred_element_type=jnp.float32)


def on_device(gate, up, cot, flags, owner, mult, pieces):
    _, slots, tok, cols = gate.shape
    feats = cot.shape[3]
    dp = lax.axis_size("dp")
    mp = lax.axis_size("mp")
    outer, inner = mp, dp // mp
    i = lax.axis_index("dp")
    z = i // inner
    x = i % inner
    ids = jnp.arange(pieces.shape[0], dtype=jnp.int32)
    tiles = jnp.sum(jnp.where(owner[0][:, None] == ids[None, :], pieces[None, :], 0), axis=1)
    live = tiles * TILE
    weight = flags[0].astype(jnp.float32) * mult[0].astype(jnp.float32)
    tokens = jnp.sum(weight * live.astype(jnp.float32))
    rows = slots * tok
    block = feats // inner
    scaled = (cot[0].astype(jnp.float32) * weight[:, None, None]).astype(jnp.bfloat16).reshape(rows, feats)
    if inner == 2:
        swapped = jnp.concatenate([scaled[:, block:], scaled[:, :block]], axis=1)
        scaled = jnp.where(x == 0, scaled, swapped)
    both = ("dp", "mp")
    perm = []
    for a in range(outer):
        for b in range(inner):
            for m in range(mp):
                perm.append(((a * inner + b) * mp + m, (m * inner + b) * mp + (a ^ m)))
    moved = lax.ppermute(scaled, both, perm)
    cots = lax.all_gather(moved, "mp", axis=0, tiled=True)
    total = lax.psum(tokens, "dp")

    def perm_z(pairs):
        return [(a * inner + b, c * inner + b) for a, c in pairs for b in range(inner)]

    sizes = [cols // CHUNKS] * CHUNKS
    lo = 0
    mask = (jnp.arange(tok, dtype=jnp.int32)[None, :] < live[:, None])
    outs = []
    for c, w in enumerate(sizes):
        g = gate[0, :, :, lo : lo + w].astype(jnp.float32)
        u = up[0, :, :, lo : lo + w].astype(jnp.float32)
        lo += w
        h = (jax.nn.silu(g) * u * mask[:, :, None].astype(jnp.float32)).astype(jnp.bfloat16).reshape(rows, w)
        ha = lax.ppermute(h, "dp", perm_z([(0, 1), (1, 0), (2, 3), (3, 2)]))
        hq = lax.ppermute(h, "dp", perm_z([(0, 2), (2, 0), (1, 3), (3, 1)]))
        hf1 = lax.ppermute(h, "dp", perm_z([(1, 2), (2, 1)]))
        hf2 = lax.ppermute(hq, "dp", perm_z([(1, 0), (2, 3)]))
        hf = jnp.where((z == 1) | (z == 2), hf1, hf2)
        hs = jnp.concatenate([h, ha, hq, hf], axis=0)
        if inner == 2:
            send = project(cots[:, block:], hs).astype(jnp.bfloat16)
            got = lax.ppermute(send, "dp", [(d, d ^ 1) for d in range(dp)])
            outs.append((project(cots[:, :block], hs) + got.astype(jnp.float32)) / total)
        else:
            partial = project(cots, hs).astype(jnp.bfloat16).reshape(inner, block, w)
            groups = [[a * inner + b for b in range(inner)] for a in range(outer)]
            got = lax.all_to_all(partial, "dp", 0, 0, axis_index_groups=groups, tiled=True)
            outs.append(jnp.sum(got.astype(jnp.float32), axis=0) / total)
    return jnp.concatenate(outs, axis=1)


def solution(mesh):
    return jax.shard_map(
        on_device,
        mesh=mesh,
        in_specs=(
            P("dp", None, None, "mp"),
            P("dp", None, None, "mp"),
            P("dp", None, None, "mp"),
            P("dp"),
            P("dp", None),
            P("dp", None),
            P(),
        ),
        out_specs=P("dp", "mp"),
        check_vma=False,
    )
```
